32 devices in a mesh: grp: 2 (over y), hist: 4 (over z), chan: 2 (over x), seq: 2 (over core).
Axes of the slice: x: 2, y: 2, z: 4, core: 2. Of those that a mesh axis runs over, the one named last changes fastest.
Arguments:
- history: bfloat16 [16, 2048, 4096], P(('grp', 'seq'), 'hist', 'chan'), parts along dimension 0, may hold values from -6 to 6
- filter_taps: bfloat16 [4096, 4096], P(('grp', 'hist'), 'chan'), parts along dimension 0, may hold values from -0.125 to 0.125
- skip_gain: float32 [8192], P(('grp', 'chan')), parts along dimension 0, may hold values from -4 to 4
- gate_values: bfloat16 [16, 64, 4096], P(('grp', 'seq'), 'hist', 'chan'), parts along dimension 0, may hold values from -6 to 6
Outputs:
- output: bfloat16 [16, 64, 4096], P(('grp', 'seq'), 'hist', 'chan'), parts along dimension 0
The draws below stay inside these ranges and needn't reach their ends.
There are 2 independent parts, one for each index of `grp`. The reference program is written for one: setup_inputs(seed, part) draws one part's arguments, and reference() takes and returns one part's arrays. A program takes and returns all parts, laid end to end along the dimension named above; each array names one. Nothing has to cross between parts.
All inputs are finite; a program needn't handle non-finite values.
Results may differ from the reference program's by a relative error of at most 0.0085.
Values may be sent and summed in bfloat16 or wider, within the bound.
No kernel may reach another device: no remote copies, remote signals or barrier semaphores. Data moves between devices by JAX's collectives and lax.ppermute only.
A program may use at most 192 MiB of HBM per device.

```python
import jax
import jax.numpy as jnp
from jax import lax

CH = 4096
SEQS = 8
NEW = 64
TOTAL = 2048


def steps_of(rng, dims, pieces, smallest, top_value):
    def one(axis_at, parts):
        steps = jax.random.uniform(jax.random.fold_in(jax.random.fold_in(rng, 6), axis_at), (parts,), jnp.float32, smallest / len(pieces), top_value / len(pieces))
        return jnp.repeat(jnp.exp(steps), dims[axis_at] // parts).reshape((-1,) + (1,) * (len(dims) - axis_at - 1))

    level = one(*pieces[0])
    for cut in pieces[1:]:
        level = level * one(*cut)
    return level


def scatter_about(rng, shape, spread, reach, pieces=(), dtype=jnp.bfloat16):
    loudness = steps_of(rng, shape, pieces, -0.22, 0.18) if pieces else 1.0
    values = jax.random.normal(rng, shape, jnp.float32) * spread * loudness
    return jnp.minimum(jnp.maximum(values, -reach), reach).astype(dtype)


def setup_inputs(seed: int = 0, part: int = 0) -> dict:
    arg_keys = jax.random.split(jax.random.key(seed), 5)
    part_keys = jax.random.split(jax.random.fold_in(arg_keys[4], part), 5)
    return {
        "history": scatter_about(part_keys[0], (SEQS, TOTAL, CH), 1.0, 6.0, ((0, 2), (1, 4), (2, 2))),
        "filter_taps": scatter_about(part_keys[1], (TOTAL, CH), TOTAL ** -0.5, 0.125, ((0, 4), (1, 2))),
        "skip_gain": scatter_about(part_keys[2], (CH,), 1.0, 4.0, ((0, 2),), jnp.float32),
        "gate_values": scatter_about(part_keys[3], (SEQS, NEW, CH), 1.0, 6.0, ((0, 2), (1, 4), (2, 2))),
    }


def reference(history, filter_taps, skip_gain, gate_values):
    full_len = history.shape[1]
    fft_len = 2 * full_len
    channels = history.shape[2]
    width = min(256, channels)
    blocks = channels // width
    inputs = history.reshape(history.shape[0], full_len, blocks, width).transpose(2, 0, 1, 3)
    filters = filter_taps[::-1].reshape(full_len, blocks, width).transpose(1, 0, 2)

    def per_block(pair):
        values, taps = pair
        spectrum_in = jnp.fft.rfft(values.astype(jnp.float32), n=fft_len, axis=1)
        spectrum_taps = jnp.fft.rfft(taps.astype(jnp.float32), n=fft_len, axis=0)
        result = jnp.fft.irfft(spectrum_in * spectrum_taps[None], n=fft_len, axis=1)
        return result[:, full_len - NEW:full_len].astype(jnp.float32)

    conv = lax.map(per_block, (inputs, filters))
    conv = conv.transpose(1, 2, 0, 3).reshape(history.shape[0], NEW, channels)
    newest = history[:, full_len - NEW:, :].astype(jnp.float32)
    mixed = conv + skip_gain[None, None, :] * newest
    return (gate_values.astype(jnp.float32) * mixed).astype(jnp.bfloat16)
```

```python
import functools

import jax
import jax.numpy as jnp
import numpy as np
from jax import lax
from jax.experimental import pallas as pl
from jax.experimental.pallas import tpu as pltpu
from jax.sharding import PartitionSpec as P

LANES = 256
BLOCK = 128


def tables(block, new):
    length = block + new
    bins = length // 2
    freq = np.arange(bins)[:, None] + 0.5
    step = 2.0 * np.pi / length

    def pair(positions):
        angle = step * freq * positions[None, :]
        return np.concatenate([np.cos(angle), np.sin(angle)], axis=0)

    taps = pair(np.arange(length))
    back = pair(new - 1 - np.arange(new)).T * (2.0 / length)
    back[:, bins:] *= -1.0
    return taps, back


def conv_body(meta, hist, taps, rim, gain, fwd, back, *outs):
    seqs, rows, lanes = hist.shape
    new = rim.shape[0]
    length = fwd.shape[1]
    block = length - new
    bins = length // 2
    count = rows // block
    share = new // len(outs)
    fwd_taps = fwd[...]
    fwd_hist = fwd[:, :block]
    back_table = back[0]
    flag = (meta[0] == len(outs) - 1).astype(jnp.float32)
    scale = gain[...] * flag
    spectra = []
    for q in range(count):
        if q + 1 < count:
            window = taps[q * block : q * block + length, :]
        else:
            window = jnp.concatenate([taps[q * block :, :], rim[...]], axis=0)
        spectra.append(jnp.dot(fwd_taps, window, preferred_element_type=jnp.float32))
    for b in range(seqs):
        real = jnp.zeros((bins, lanes), jnp.float32)
        imag = jnp.zeros((bins, lanes), jnp.float32)
        for q in range(count):
            data = jnp.dot(
                fwd_hist,
                hist[b, q * block : (q + 1) * block, :],
                preferred_element_type=jnp.float32,
            )
            dc, ds = data[:bins], data[bins:]
            tc, ts = spectra[q][:bins], spectra[q][bins:]
            real = real + (dc * tc + ds * ts)
            imag = imag + (ds * tc - dc * ts)
        both = jnp.concatenate([real, imag], axis=0).astype(jnp.bfloat16)
        part = jnp.dot(back_table, both, preferred_element_type=jnp.float32)
        newest = hist[b, rows - new :, :].astype(jnp.float32)
        for j, out in enumerate(outs):
            first = (j - 1) % len(outs) * share
            direct = scale * newest[first : first + share]
            piece = part[j * share : (j + 1) * share] + direct
            out[b] = piece.astype(out.dtype)


def conv_chunk(meta, history, taps, rim, gain, fwd, back, tiles, ranks):
    seqs, rows, _ = history.shape
    new = rim.shape[0]
    share = new // ranks
    width = tiles * LANES
    shapes = [
        jax.ShapeDtypeStruct((seqs, share, width), jnp.bfloat16 if j else jnp.float32)
        for j in range(ranks)
    ]
    flops = 2 * width * fwd.shape[0] * rows * (seqs + 1)
    spec = pltpu.PrefetchScalarGridSpec(
        num_scalar_prefetch=1,
        grid=(tiles,),
        in_specs=[
            pl.BlockSpec((seqs, rows, LANES), lambda t, m: (0, 0, m[1] + t)),
            pl.BlockSpec((rows, LANES), lambda t, m: (0, m[1] + t)),
            pl.BlockSpec((new, LANES), lambda t, m: (0, m[1] + t)),
            pl.BlockSpec((1, LANES), lambda t, m: (0, m[1] + t)),
            pl.BlockSpec(fwd.shape, lambda t, m: (0, 0)),
            pl.BlockSpec((1,) + back.shape[1:], lambda t, m: (m[0], 0, 0)),
        ],
        out_specs=[
            pl.BlockSpec((seqs, share, LANES), lambda t, m: (0, 0, t)) for _ in shapes
        ],
    )
    return pl.pallas_call(
        conv_body,
        grid_spec=spec,
        out_shape=shapes,
        cost_estimate=pl.CostEstimate(
            flops=flops,
            transcendentals=0,
            bytes_accessed=2 * width * rows * (seqs + 1),
        ),
        name="conv_chunk",
    )(meta, history, taps, rim, gain, fwd, back)


def chunk_tiles(total):
    sizes = []
    left = total
    while left:
        size = min(left, 1 if not sizes else 2)
        sizes.append(size)
        left -= size
    return sizes


def body(history, filter_taps, skip_gain, gate_values):
    ranks = lax.axis_size("hist")
    rank = lax.axis_index("hist").astype(jnp.int32)
    new = gate_values.shape[1] * ranks
    share = gate_values.shape[1]
    channels = history.shape[2]
    block = min(BLOCK, history.shape[1])
    taps_table, back_table = tables(block, new)
    fwd = jnp.asarray(taps_table, jnp.bfloat16)
    turned = np.stack([np.roll(back_table, -share * z, axis=0) for z in range(ranks)])
    back = jnp.asarray(turned, jnp.bfloat16)
    rim = lax.ppermute(
        filter_taps[:new], "hist", [(source, source - 1) for source in range(1, ranks)]
    )
    gain = skip_gain[None, :]
    pieces = []
    start = 0
    for tiles in chunk_tiles(channels // LANES):
        meta = jnp.stack([rank, jnp.int32(start)])
        parts = conv_chunk(meta, history, filter_taps, rim, gain, fwd, back, tiles, ranks)
        total = parts[0]
        for j in range(1, ranks):
            got = lax.ppermute(
                parts[j], "hist", [(source, (source + j) % ranks) for source in range(ranks)]
            )
            total = total + got.astype(jnp.float32)
        lo, hi = start * LANES, (start + tiles) * LANES
        gate = gate_values[:, :, lo:hi].astype(jnp.float32)
        pieces.append((gate * total).astype(jnp.bfloat16))
        start += tiles
    return jnp.concatenate(pieces, axis=2)


def solution(mesh):
    placed = (
        P(("grp", "seq"), "hist", "chan"),
        P(("grp", "hist"), "chan"),
        P(("grp", "chan")),
        P(("grp", "seq"), "hist", "chan"),
    )
    return jax.shard_map(
        body,
        mesh=mesh,
        in_specs=placed,
        out_specs=P(("grp", "seq"), "hist", "chan"),
        check_vma=False,
    )
```

```python
import functools

import jax
import jax.numpy as jnp
import numpy as np
from jax import lax
from jax.experimental import pallas as pl
from jax.experimental.pallas import tpu as pltpu
from jax.sharding import PartitionSpec as P


LANES = 256
BLOCK = 128


def tables(block, new):
    length = block + new
    bins = length // 2
    freq = np.arange(bins)[:, None] + 0.5
    step = 2.0 * np.pi / length

    def pair(positions):
        angle = step * freq * positions[None, :]
        return np.concatenate([np.cos(angle), np.sin(angle)], axis=0)

    taps = pair(np.arange(length))
    back = pair(new - 1 - np.arange(new)).T * (2.0 / length)
    back[:, bins:] *= -1.0
    return taps, back


def conv_body(meta, hist, taps, gain, fwd, back, rim, keep, send, *, base, rim_base, owners):
    seqs, rows, _ = hist.shape
    new = rim.shape[0]
    length = fwd.shape[1]
    block = length - new
    bins = length // 2
    count = rows // block
    share = new // len(owners)
    flag = (meta[0] == len(owners) - 1).astype(jnp.float32)

    def tile(t, carry):
        here = pl.ds(pl.multiple_of((base + t) * LANES, LANES), LANES)
        there = pl.ds(pl.multiple_of(t * LANES, LANES), LANES)
        rim_at = pl.ds(pl.multiple_of((base - rim_base + t) * LANES, LANES), LANES)
        fwd_taps = fwd[...]
        fwd_hist = fwd[:, :block]
        back_table = back[meta[0]]
        scale = gain[:, here] * flag
        spectra = []
        for q in range(count):
            if q + 1 < count:
                window = taps[q * block : q * block + length, here]
            else:
                window = jnp.concatenate([taps[q * block :, here], rim[:, rim_at]], axis=0)
            spectra.append(jnp.dot(fwd_taps, window, preferred_element_type=jnp.float32))
        for b in range(seqs):
            real = jnp.zeros((bins, LANES), jnp.float32)
            imag = jnp.zeros((bins, LANES), jnp.float32)
            for q in range(count):
                data = jnp.dot(
                    fwd_hist,
                    hist[b, q * block : (q + 1) * block, here],
                    preferred_element_type=jnp.float32,
                )
                dc, ds = data[:bins], data[bins:]
                tc, ts = spectra[q][:bins], spectra[q][bins:]
                real = real + (dc * tc + ds * ts)
                imag = imag + (ds * tc - dc * ts)
            both = jnp.concatenate([real, imag], axis=0).astype(jnp.bfloat16)
            part = jnp.dot(back_table, both, preferred_element_type=jnp.float32)
            newest = hist[b, rows - new :, here].astype(jnp.float32)
            for k, owner in enumerate(owners):
                direct = scale * newest[owner * share : (owner + 1) * share]
                piece = part[k * share : (k + 1) * share] + direct
                out = keep if k < len(owners) // 2 else send
                at = k % max(1, len(owners) // 2) * share
                out[b, at : at + share, there] = piece.astype(out.dtype)
        return carry

    lax.fori_loop(0, keep.shape[2] // LANES, tile, 0)


def stage_body(*refs):
    count = len(refs) // 2
    arrays, copies, done = refs[:count], refs[count:-1], refs[-1]
    moves = [
        pltpu.make_async_copy(arrays[i], copies[i], done.at[i]) for i in range(count)
    ]
    for move in moves:
        move.start()
    for move in moves:
        move.wait()


def stage(*arrays):
    return pl.pallas_call(
        stage_body,
        in_specs=[pl.BlockSpec(memory_space=pltpu.HBM)] * len(arrays),
        out_specs=[pl.BlockSpec(memory_space=pltpu.VMEM)] * len(arrays),
        out_shape=[pltpu.VMEM(a.shape, a.dtype) for a in arrays],
        scratch_shapes=[pltpu.SemaphoreType.DMA((len(arrays),))],
        compiler_params=pltpu.CompilerParams(vmem_limit_bytes=16 << 20),
        name="stage",
    )(*[pltpu.with_memory_space_constraint(a, pltpu.HBM) for a in arrays])


def conv_chunk(meta, staged, rim, base, rim_base, tiles, owners):
    history, _, _, fwd, _ = staged
    seqs, rows, _ = history.shape
    half = rim.shape[0] // 2
    width = tiles * LANES
    vmem = pl.BlockSpec(memory_space=pltpu.VMEM)
    return pl.pallas_call(
        functools.partial(conv_body, base=base, rim_base=rim_base, owners=owners),
        in_specs=[pl.BlockSpec(memory_space=pltpu.SMEM)] + [vmem] * 6,
        out_specs=[vmem] * 2,
        out_shape=[
            jax.ShapeDtypeStruct((seqs, half, width), jnp.float32),
            jax.ShapeDtypeStruct((seqs, half, width), jnp.bfloat16),
        ],
        cost_estimate=pl.CostEstimate(
            flops=2 * width * fwd.shape[0] * rows * (seqs + 1),
            transcendentals=0,
            bytes_accessed=2 * width * rows * (seqs + 1),
        ),
        compiler_params=pltpu.CompilerParams(vmem_limit_bytes=16 << 20),
        name="conv_chunk",
    )(meta, *staged, rim)


def chunk_tiles(total):
    sizes = []
    left = total
    while left:
        size = min(left, 1 if not sizes else 2)
        sizes.append(size)
        left -= size
    return sizes


def swapped(ranks):
    order = [0]
    step = ranks // 2
    while step:
        order += [step ^ value for value in order]
        step //= 2
    return order


def exchange(value, bit, ranks):
    return lax.ppermute(value, "hist", [(z, z ^ bit) for z in range(ranks)])


def body(history, filter_taps, skip_gain, gate_values):
    ranks = lax.axis_size("hist")
    rank = lax.axis_index("hist").astype(jnp.int32)
    share = gate_values.shape[1]
    new = share * ranks
    channels = history.shape[2]
    block = min(BLOCK, history.shape[1])
    taps_table, back_table = tables(block, new)
    fwd = jnp.asarray(taps_table, jnp.bfloat16)
    order = swapped(ranks)
    by_owner = back_table.reshape(ranks, share, -1)
    turned = np.stack(
        [np.concatenate([by_owner[z ^ j] for j in order]) for z in range(ranks)]
    )
    back = jnp.asarray(turned, jnp.bfloat16)
    owners = [(ranks - 1) ^ j for j in order]
    meta = rank[None]
    sizes = chunk_tiles(channels // LANES)
    toward = [(source, source - 1) for source in range(1, ranks)]
    split = sizes[0] * LANES
    rims = []
    for part in (slice(0, split), slice(split, None)):
        rims.append(lax.ppermute(filter_taps[:new, part], "hist", toward))
    staged = stage(history, filter_taps, skip_gain[None, :], fwd, back)
    pieces = []
    start = 0
    for index, tiles in enumerate(sizes):
        keep, send = conv_chunk(
            meta,
            staged,
            rims[min(index, 1)],
            start,
            sizes[0] if index else 0,
            tiles,
            owners,
        )
        bit = 1
        while bit < ranks:
            got = exchange(send, bit, ranks)
            total = keep + got.astype(jnp.float32)
            half = total.shape[1] // 2
            keep, send = total[:, :half], total[:, half:].astype(jnp.bfloat16)
            bit *= 2
        lo, hi = start * LANES, (start + tiles) * LANES
        gate = gate_values[:, :, lo:hi].astype(jnp.float32)
        pieces.append((gate * total).astype(jnp.bfloat16))
        start += tiles
    return jnp.concatenate(pieces, axis=2)


def solution(mesh):
    placed = (
        P(("grp", "seq"), "hist", "chan"),
        P(("grp", "hist"), "chan"),
        P(("grp", "chan")),
        P(("grp", "seq"), "hist", "chan"),
    )
    return jax.shard_map(
        body,
        mesh=mesh,
        in_specs=placed,
        out_specs=P(("grp", "seq"), "hist", "chan"),
        check_vma=False,
    )
```

```python
import functools

import jax
import jax.numpy as jnp
import numpy as np
from jax import lax
from jax.experimental import pallas as pl
from jax.experimental.pallas import tpu as pltpu
from jax.sharding import PartitionSpec as P


LANES = 256
BLOCK = 128
CHUNKS = 3
GROUP = 16


def tables(block, new):
    length = block + new
    bins = length // 2
    freq = np.arange(bins)[:, None] + 0.5
    step = 2.0 * np.pi / length

    def pair(positions):
        angle = step * freq * positions[None, :]
        return np.concatenate([np.cos(angle), np.sin(angle)], axis=0)

    taps = pair(np.arange(length))
    back = pair(new - 1 - np.arange(new)).T * (2.0 / length)
    back[:, bins:] *= -1.0
    return taps, back


def conv_body(
    meta, hist, taps, gain, fwd, back, rim, keep, send, spectra, *, base, rim_base, owners
):
    seqs, rows, _ = hist.shape
    new = rim.shape[0]
    length = fwd.shape[1]
    block = length - new
    bins = length // 2
    count = rows // block
    share = new // len(owners)
    flag = (meta[0] == len(owners) - 1).astype(jnp.float32)

    def tile(t, carry):
        here = pl.ds(pl.multiple_of((base + t) * LANES, LANES), LANES)
        there = pl.ds(pl.multiple_of(t * LANES, LANES), LANES)
        rim_at = pl.ds(pl.multiple_of((base - rim_base + t) * LANES, LANES), LANES)
        fwd_taps = fwd[...]
        fwd_hist = fwd[:, :block]
        back_table = back[meta[0]]
        scale = gain[:, here] * flag

        def forward(b):
            return [
                jnp.dot(
                    fwd_hist,
                    hist[b, q * block : (q + 1) * block, here],
                    preferred_element_type=jnp.float32,
                )
                for q in range(count)
            ]

        def combine(data):
            real, imag = [], []
            for f in range(0, bins, GROUP):
                re = im = None
                for q in range(count):
                    dc, ds = data[q][f : f + GROUP], data[q][bins + f : bins + f + GROUP]
                    tc = spectra[q, f : f + GROUP, :]
                    ts = spectra[q, bins + f : bins + f + GROUP, :]
                    now_re, now_im = dc * tc + ds * ts, ds * tc - dc * ts
                    re = now_re if re is None else re + now_re
                    im = now_im if im is None else im + now_im
                real.append(re.astype(jnp.bfloat16))
                imag.append(im.astype(jnp.bfloat16))
            both = jnp.concatenate(real + imag, axis=0)
            return jnp.dot(back_table, both, preferred_element_type=jnp.float32)

        def finish(b, part):
            newest = hist[b, rows - new :, here].astype(jnp.float32)
            for k, owner in enumerate(owners):
                direct = scale * newest[owner * share : (owner + 1) * share]
                piece = part[k * share : (k + 1) * share] + direct
                out = keep if k < len(owners) // 2 else send
                at = k % max(1, len(owners) // 2) * share
                out[b, at : at + share, there] = piece.astype(out.dtype)

        for q in range(count):
            if q + 1 < count:
                window = taps[q * block : q * block + length, here]
            else:
                window = jnp.concatenate([taps[q * block :, here], rim[:, rim_at]], axis=0)
            spectra[q] = jnp.dot(fwd_taps, window, preferred_element_type=jnp.float32)
        data = forward(0)
        part = None
        for b in range(seqs):
            after = forward(b + 1) if b + 1 < seqs else None
            now = combine(data)
            if part is not None:
                finish(b - 1, part)
            part, data = now, after
        finish(seqs - 1, part)
        return carry

    lax.fori_loop(0, keep.shape[2] // LANES, tile, 0)


def stage_body(*refs):
    count = len(refs) // 2
    arrays, copies, done = refs[:count], refs[count:-1], refs[-1]
    moves = [
        pltpu.make_async_copy(arrays[i], copies[i], done.at[i]) for i in range(count)
    ]
    for move in moves:
        move.start()
    for move in moves:
        move.wait()


def stage(*arrays):
    return pl.pallas_call(
        stage_body,
        in_specs=[pl.BlockSpec(memory_space=pltpu.HBM)] * len(arrays),
        out_specs=[pl.BlockSpec(memory_space=pltpu.VMEM)] * len(arrays),
        out_shape=[pltpu.VMEM(a.shape, a.dtype) for a in arrays],
        scratch_shapes=[pltpu.SemaphoreType.DMA((len(arrays),))],
        compiler_params=pltpu.CompilerParams(vmem_limit_bytes=16 << 20),
        name="stage",
    )(*[pltpu.with_memory_space_constraint(a, pltpu.HBM) for a in arrays])


def conv_chunk(meta, staged, rim, base, rim_base, tiles, owners):
    history, _, _, fwd, _ = staged
    seqs, rows, _ = history.shape
    half = rim.shape[0] // 2
    width = tiles * LANES
    vmem = pl.BlockSpec(memory_space=pltpu.VMEM)
    return pl.pallas_call(
        functools.partial(conv_body, base=base, rim_base=rim_base, owners=owners),
        in_specs=[pl.BlockSpec(memory_space=pltpu.SMEM)] + [vmem] * 6,
        out_specs=[vmem] * 2,
        scratch_shapes=[
            pltpu.VMEM((rows // (fwd.shape[1] - rim.shape[0]), fwd.shape[0], LANES), jnp.float32)
        ],
        out_shape=[
            jax.ShapeDtypeStruct((seqs, half, width), jnp.float32),
            jax.ShapeDtypeStruct((seqs, half, width), jnp.bfloat16),
        ],
        cost_estimate=pl.CostEstimate(
            flops=2 * width * fwd.shape[0] * rows * (seqs + 1),
            transcendentals=0,
            bytes_accessed=2 * width * rows * (seqs + 1),
        ),
        compiler_params=pltpu.CompilerParams(vmem_limit_bytes=16 << 20),
        name="conv_chunk",
    )(meta, *staged, rim)


def chunk_tiles(total):
    parts = min(CHUNKS, total)
    return [total // parts + (index < total % parts) for index in range(parts)]


def swapped(ranks):
    order = [0]
    step = ranks // 2
    while step:
        order += [step ^ value for value in order]
        step //= 2
    return order


def exchange(value, bit, ranks):
    return lax.ppermute(value, "hist", [(z, z ^ bit) for z in range(ranks)])


def body(history, filter_taps, skip_gain, gate_values):
    ranks = lax.axis_size("hist")
    rank = lax.axis_index("hist").astype(jnp.int32)
    share = gate_values.shape[1]
    new = share * ranks
    channels = history.shape[2]
    block = min(BLOCK, history.shape[1])
    taps_table, back_table = tables(block, new)
    fwd = jnp.asarray(taps_table, jnp.bfloat16)
    order = swapped(ranks)
    by_owner = back_table.reshape(ranks, share, -1)
    turned = np.stack(
        [np.concatenate([by_owner[z ^ j] for j in order]) for z in range(ranks)]
    )
    back = jnp.asarray(turned, jnp.bfloat16)
    owners = [(ranks - 1) ^ j for j in order]
    meta = rank[None]
    sizes = chunk_tiles(channels // LANES)
    toward = [(source, source - 1) for source in range(1, ranks)]
    split = sizes[0] * LANES
    rims = []
    for part in (slice(0, split), slice(split, None)):
        rims.append(lax.ppermute(filter_taps[:new, part], "hist", toward))
    staged = stage(history, filter_taps, skip_gain[None, :], fwd, back)
    pieces = []
    start = 0
    for index, tiles in enumerate(sizes):
        keep, send = conv_chunk(
            meta,
            staged,
            rims[min(index, 1)],
            start,
            sizes[0] if index else 0,
            tiles,
            owners,
        )
        bit = 1
        while bit < ranks:
            got = exchange(send, bit, ranks)
            total = keep + got.astype(jnp.float32)
            half = total.shape[1] // 2
            keep, send = total[:, :half], total[:, half:].astype(jnp.bfloat16)
            bit *= 2
        lo, hi = start * LANES, (start + tiles) * LANES
        gate = gate_values[:, :, lo:hi].astype(jnp.float32)
        pieces.append((gate * total).astype(jnp.bfloat16))
        start += tiles
    return jnp.concatenate(pieces, axis=2)


def solution(mesh):
    placed = (
        P(("grp", "seq"), "hist", "chan"),
        P(("grp", "hist"), "chan"),
        P(("grp", "chan")),
        P(("grp", "seq"), "hist", "chan"),
    )
    return jax.shard_map(
        body,
        mesh=mesh,
        in_specs=placed,
        out_specs=P(("grp", "seq"), "hist", "chan"),
        check_vma=False,
    )
```

```python
import functools

import jax
import jax.numpy as jnp
import numpy as np
from jax import lax
from jax.experimental import pallas as pl
from jax.experimental.pallas import tpu as pltpu
from jax.sharding import PartitionSpec as P


LANES = 256
BLOCK = 128
CHUNKS = 3
STRAIGHT = 4
DIRECT = ()
GROUP = 16


def tables(block, new):
    length = block + new
    bins = length // 2
    freq = np.arange(bins)[:, None] + 0.5
    step = 2.0 * np.pi / length

    def pair(positions):
        angle = step * freq * positions[None, :]
        return np.concatenate([np.cos(angle), np.sin(angle)], axis=0)

    taps = pair(np.arange(length))
    back = pair(new - 1 - np.arange(new)).T * (2.0 / length)
    back[:, bins:] *= -1.0
    return taps, back


def moves_in(sources, targets, done, first, count):
    moves = []
    for source, target in zip(sources, targets):
        for t in range(count):
            lead = (slice(None),) * (len(source.shape) - 1)
            there = lead + (pl.ds((first + t) * LANES, LANES),)
            here = lead + (pl.ds(t * LANES, LANES),)
            moves.append(
                pltpu.make_async_copy(source.at[there], target.at[here], done.at[len(moves)])
            )
    return moves


def conv_body(meta, hist, taps, gain, fwd, back, rim, *refs, first, tiles, base, owners):
    if base is None:
        sources, refs = (), refs
        outs, (spectra,) = refs[:-1], refs[-1:]
    else:
        sources, refs = refs[:2], refs[2:]
        outs, targets, (spectra, done) = refs[:-4], refs[-4:-2], refs[-2:]
        later = moves_in(sources, targets, done, base, targets[0].shape[2] // LANES)
        for move in later:
            move.start()
    seqs, rows, _ = hist.shape
    new = rim.shape[0]
    length = fwd.shape[1]
    block = length - new
    bins = length // 2
    count = rows // block
    share = new // len(owners)
    flag = (meta[0] == len(owners) - 1).astype(jnp.float32)
    hist_at, rim_at, gain_at = first

    def tile(t, carry):
        here = pl.ds(pl.multiple_of((hist_at + t) * LANES, LANES), LANES)
        near = pl.ds(pl.multiple_of((rim_at + t) * LANES, LANES), LANES)
        there = pl.ds(pl.multiple_of(t * LANES, LANES), LANES)
        fwd_taps = fwd[...]
        fwd_hist = fwd[:, :block]
        back_table = back[meta[0]]
        scale = gain[:, pl.ds(pl.multiple_of((gain_at + t) * LANES, LANES), LANES)] * flag

        def forward(b):
            return [
                jnp.dot(
                    fwd_hist,
                    hist[b, q * block : (q + 1) * block, here],
                    preferred_element_type=jnp.float32,
                )
                for q in range(count)
            ]

        def combine(data):
            real, imag = [], []
            for f in range(0, bins, GROUP):
                re = im = None
                for q in range(count):
                    dc, ds = data[q][f : f + GROUP], data[q][bins + f : bins + f + GROUP]
                    tc = spectra[q, f : f + GROUP, :]
                    ts = spectra[q, bins + f : bins + f + GROUP, :]
                    now_re, now_im = dc * tc + ds * ts, ds * tc - dc * ts
                    re = now_re if re is None else re + now_re
                    im = now_im if im is None else im + now_im
                real.append(re.astype(jnp.bfloat16))
                imag.append(im.astype(jnp.bfloat16))
            both = jnp.concatenate(real + imag, axis=0)
            return jnp.dot(back_table, both, preferred_element_type=jnp.float32)

        def finish(b, part):
            newest = hist[b, rows - new :, here].astype(jnp.float32)
            for k, owner in enumerate(owners):
                direct = scale * newest[owner * share : (owner + 1) * share]
                piece = part[k * share : (k + 1) * share] + direct
                out = outs[k * len(outs) // len(owners)]
                at = k % (len(owners) // len(outs)) * share
                out[b, at : at + share, there] = piece.astype(out.dtype)

        for q in range(count):
            if q + 1 < count:
                window = taps[q * block : q * block + length, here]
            else:
                window = jnp.concatenate([taps[q * block :, here], rim[:, near]], axis=0)
            spectra[q] = jnp.dot(fwd_taps, window, preferred_element_type=jnp.float32)
        data = forward(0)
        part = None
        for b in range(seqs):
            after = forward(b + 1) if b + 1 < seqs else None
            now = combine(data)
            if part is not None:
                finish(b - 1, part)
            part, data = now, after
        finish(seqs - 1, part)
        return carry

    lax.fori_loop(0, tiles, tile, 0)
    if base is not None:
        for move in later:
            move.wait()


def stage_body(meta, *refs, tiles):
    del meta
    count = len(refs) // 2 - 1
    arrays, copies, (done, whole) = refs[:count], refs[count:-2], refs[-2:]
    moves = moves_in(arrays[:2], copies[:2], done, 0, tiles)
    for i in range(2, count):
        moves.append(pltpu.make_async_copy(arrays[i], copies[i], whole.at[i]))
    for move in moves:
        move.start()
    for move in moves:
        move.wait()


def in_hbm(*arrays):
    return [pltpu.with_memory_space_constraint(a, pltpu.HBM) for a in arrays]


def stage(meta, history, taps, *rest, tiles):
    width = tiles * LANES
    arrays = (history, taps) + rest
    shapes = [a.shape[:-1] + (width,) for a in arrays[:2]] + [a.shape for a in rest]
    return pl.pallas_call(
        functools.partial(stage_body, tiles=tiles),
        in_specs=[pl.BlockSpec(memory_space=pltpu.SMEM)]
        + [pl.BlockSpec(memory_space=pltpu.HBM)] * len(arrays),
        out_specs=[pl.BlockSpec(memory_space=pltpu.VMEM)] * len(arrays),
        out_shape=[pltpu.VMEM(d, a.dtype) for d, a in zip(shapes, arrays)],
        scratch_shapes=[
            pltpu.SemaphoreType.DMA((2 * tiles,)),
            pltpu.SemaphoreType.DMA((len(arrays),)),
        ],
        compiler_params=pltpu.CompilerParams(vmem_limit_bytes=16 << 20),
        name="stage",
    )(meta, *in_hbm(*arrays))


def conv_chunk(meta, staged, rim, first, tiles, owners, splits, later=None):
    history, _, _, fwd, _ = staged
    seqs, rows, _ = history.shape
    new = rim.shape[0]
    width = tiles * LANES
    vmem = pl.BlockSpec(memory_space=pltpu.VMEM)
    operands = [meta, *staged, rim]
    in_specs = [pl.BlockSpec(memory_space=pltpu.SMEM)] + [vmem] * 6
    out_shape = [
        jax.ShapeDtypeStruct(
            (seqs, new // splits, width), jnp.bfloat16 if k else jnp.float32
        )
        for k in range(splits)
    ]
    scratch = [
        pltpu.VMEM((rows // (fwd.shape[1] - new), fwd.shape[0], LANES), jnp.float32)
    ]
    base = None
    if later is not None:
        base = tiles
        left = later[0].shape[-1] // LANES - tiles
        operands += in_hbm(*later)
        in_specs += [pl.BlockSpec(memory_space=pltpu.HBM)] * 2
        out_shape += [
            pltpu.VMEM(a.shape[:-1] + (left * LANES,), a.dtype) for a in later
        ]
        scratch.append(pltpu.SemaphoreType.DMA((2 * left,)))
    return pl.pallas_call(
        functools.partial(conv_body, first=first, tiles=tiles, base=base, owners=owners),
        in_specs=in_specs,
        out_specs=[vmem] * len(out_shape),
        out_shape=out_shape,
        scratch_shapes=scratch,
        cost_estimate=pl.CostEstimate(
            flops=2 * width * fwd.shape[0] * rows * (seqs + 1),
            transcendentals=0,
            bytes_accessed=2 * width * rows * (seqs + 1),
        ),
        compiler_params=pltpu.CompilerParams(vmem_limit_bytes=16 << 20),
        name="conv_chunk",
    )(*operands)


def gate_body(gate, *refs, counts):
    *pieces, out = refs
    place = 0
    for count in counts:
        (keep, *got), pieces = pieces[:count], pieces[count:]
        for t in range(keep.shape[2] // LANES):
            here = slice(place * LANES, (place + 1) * LANES)
            there = slice(t * LANES, (t + 1) * LANES)
            value = keep[:, :, there]
            for piece in got:
                value = value + piece[:, :, there].astype(jnp.float32)
            scaled = gate[:, :, here].astype(jnp.float32) * value
            out[:, :, here] = scaled.astype(out.dtype)
            place = place + 1


def gated(gate, chunks):
    vmem = pl.BlockSpec(memory_space=pltpu.VMEM)
    pieces = [piece for chunk in chunks for piece in chunk]
    counts = [len(chunk) for chunk in chunks]
    return pl.pallas_call(
        functools.partial(gate_body, counts=counts),
        in_specs=[vmem] * (1 + len(pieces)),
        out_specs=vmem,
        out_shape=jax.ShapeDtypeStruct(gate.shape, gate.dtype),
        compiler_params=pltpu.CompilerParams(vmem_limit_bytes=16 << 20),
        name="gated",
    )(gate, *pieces)


def chunk_tiles(total):
    parts = min(CHUNKS, total)
    return [total // parts + (index < total % parts) for index in range(parts)]


def swapped(ranks):
    order = [0]
    step = ranks // 2
    while step:
        order += [step ^ value for value in order]
        step //= 2
    return order


def exchange(value, bit, ranks):
    return lax.ppermute(value, "hist", [(z, z ^ bit) for z in range(ranks)])


def body(history, filter_taps, skip_gain, gate_values):
    ranks = lax.axis_size("hist")
    rank = lax.axis_index("hist").astype(jnp.int32)
    share = gate_values.shape[1]
    new = share * ranks
    channels = history.shape[2]
    total = channels // LANES
    block = min(BLOCK, history.shape[1])
    taps_table, back_table = tables(block, new)
    fwd = jnp.asarray(taps_table, jnp.bfloat16)
    order = swapped(ranks)
    by_owner = back_table.reshape(ranks, share, -1)
    turned = np.stack(
        [np.concatenate([by_owner[z ^ j] for j in order]) for z in range(ranks)]
    )
    back = jnp.asarray(turned, jnp.bfloat16)
    owners = [(ranks - 1) ^ j for j in order]
    meta = rank[None]
    sizes = chunk_tiles(total)
    toward = [(source, source - 1) for source in range(1, ranks)]
    split = sizes[0] * LANES
    rims = []
    for part in (slice(0, split), slice(split, None)):
        rims.append(lax.ppermute(filter_taps[:new, part], "hist", toward))
    gain = skip_gain[None, :]
    staged = stage(meta, history, filter_taps, gain, fwd, back, tiles=sizes[0])
    chunks = []
    start = 0
    for index, tiles in enumerate(sizes):
        straight = 2 < ranks <= STRAIGHT and index in DIRECT
        splits = ranks if straight else 2
        at = start - sizes[0] if index else 0
        later = None if index or len(sizes) == 1 else (history, filter_taps)
        keep, *sends = conv_chunk(
            meta,
            staged,
            rims[min(index, 1)],
            (at, at, start),
            tiles,
            owners,
            splits,
            later,
        )
        if later is not None:
            staged = [sends[-2], sends[-1], *staged[2:]]
            sends = sends[:-2]
        got = []
        if straight:
            for k, send in enumerate(sends):
                got.append(exchange(send, order[k + 1], ranks))
        else:
            bit = 1
            while True:
                came = exchange(sends[0], bit, ranks)
                bit *= 2
                if bit >= ranks:
                    break
                summed = keep + came.astype(jnp.float32)
                half = summed.shape[1] // 2
                keep, sends = summed[:, :half], [summed[:, half:].astype(jnp.bfloat16)]
            got.append(came)
        chunks.append([keep, *got])
        start += tiles
    return gated(gate_values, chunks)


def solution(mesh):
    placed = (
        P(("grp", "seq"), "hist", "chan"),
        P(("grp", "hist"), "chan"),
        P(("grp", "chan")),
        P(("grp", "seq"), "hist", "chan"),
    )
    return jax.shard_map(
        body,
        mesh=mesh,
        in_specs=placed,
        out_specs=P(("grp", "seq"), "hist", "chan"),
        check_vma=False,
    )
```

```python
import functools

import jax
import jax.numpy as jnp
import numpy as np
from jax import lax
from jax.experimental import pallas as pl
from jax.experimental.pallas import tpu as pltpu
from jax.sharding import PartitionSpec as P


LANES = 256
BLOCK = 128
CHUNKS = 3
GROUP = 16


def tables(block, new):
    length = block + new
    bins = length // 2
    freq = np.arange(bins)[:, None] + 0.5
    step = 2.0 * np.pi / length

    def pair(positions):
        angle = step * freq * positions[None, :]
        return np.concatenate([np.cos(angle), np.sin(angle)], axis=0)

    taps = pair(np.arange(length))
    back = pair(new - 1 - np.arange(new)).T * (2.0 / length)
    back[:, bins:] *= -1.0
    return taps, back


def moves_in(sources, targets, done, first, count):
    moves = []
    for source, target in zip(sources, targets):
        for t in range(count):
            lead = (slice(None),) * (len(source.shape) - 1)
            there = lead + (pl.ds((first + t) * LANES, LANES),)
            here = lead + (pl.ds(t * LANES, LANES),)
            moves.append(
                pltpu.make_async_copy(source.at[there], target.at[here], done.at[len(moves)])
            )
    return moves


def conv_body(meta, hist, taps, gain, fwd, back, rim, *refs, first, tiles, base, owners):
    if base is None:
        sources, refs = (), refs
        outs, (spectra,) = refs[:-1], refs[-1:]
    else:
        sources, refs = refs[:2], refs[2:]
        outs, targets, (spectra, done) = refs[:-4], refs[-4:-2], refs[-2:]
        later = moves_in(sources, targets, done, base, targets[0].shape[2] // LANES)
        for move in later:
            move.start()
    seqs, rows, _ = hist.shape
    new = rim.shape[0]
    length = fwd.shape[1]
    block = length - new
    bins = length // 2
    count = rows // block
    share = new // len(owners)
    flag = (meta[0] == len(owners) - 1).astype(jnp.float32)
    hist_at, rim_at, gain_at = first

    fwd_taps = fwd[...]
    fwd_hist = fwd[:, :block]
    back_table = back[meta[0]]

    def lanes(tile):
        return slice(tile * LANES, (tile + 1) * LANES)

    def transform(t):
        for q in range(count):
            here = lanes(hist_at + t)
            if q + 1 < count:
                window = taps[q * block : q * block + length, here]
            else:
                window = jnp.concatenate(
                    [taps[q * block :, here], rim[:, lanes(rim_at + t)]], axis=0
                )
            spectra[t % 2, q] = jnp.dot(
                fwd_taps, window, preferred_element_type=jnp.float32
            )

    def forward(t, b):
        return [
            jnp.dot(
                fwd_hist,
                hist[b, q * block : (q + 1) * block, lanes(hist_at + t)],
                preferred_element_type=jnp.float32,
            )
            for q in range(count)
        ]

    def combine(t, data):
        real, imag = [], []
        for f in range(0, bins, GROUP):
            re = im = None
            for q in range(count):
                dc, ds = data[q][f : f + GROUP], data[q][bins + f : bins + f + GROUP]
                tc = spectra[t % 2, q, f : f + GROUP, :]
                ts = spectra[t % 2, q, bins + f : bins + f + GROUP, :]
                now_re, now_im = dc * tc + ds * ts, ds * tc - dc * ts
                re = now_re if re is None else re + now_re
                im = now_im if im is None else im + now_im
            real.append(re.astype(jnp.bfloat16))
            imag.append(im.astype(jnp.bfloat16))
        both = jnp.concatenate(real + imag, axis=0)
        return jnp.dot(back_table, both, preferred_element_type=jnp.float32)

    def finish(t, b, part):
        scale = gain[:, lanes(gain_at + t)] * flag
        newest = hist[b, rows - new :, lanes(hist_at + t)].astype(jnp.float32)
        for k, owner in enumerate(owners):
            direct = scale * newest[owner * share : (owner + 1) * share]
            piece = part[k * share : (k + 1) * share] + direct
            out = outs[k * len(outs) // len(owners)]
            at = k % (len(owners) // len(outs)) * share
            out[b, at : at + share, lanes(t)] = piece.astype(out.dtype)

    def compute():
        steps = [(t, b) for t in range(tiles) for b in range(seqs)]
        transform(0)
        data = forward(*steps[0])
        last = None
        for index, (t, b) in enumerate(steps):
            after = None
            if index + 1 < len(steps):
                if b == seqs // 2 and t + 1 < tiles:
                    transform(t + 1)
                after = forward(*steps[index + 1])
            now = combine(t, data)
            if last is not None:
                finish(*last)
            last, data = (t, b, now), after
        finish(*last)

    if base is None:
        compute()
        return
    pl.when(meta[0] >= 0)(compute)
    for move in later:
        move.wait()


def stage_body(meta, *refs, tiles):
    del meta
    count = len(refs) // 2 - 1
    arrays, copies, (done, whole) = refs[:count], refs[count:-2], refs[-2:]
    moves = moves_in(arrays[:2], copies[:2], done, 0, tiles)
    for i in range(2, count):
        moves.append(pltpu.make_async_copy(arrays[i], copies[i], whole.at[i]))
    for move in moves:
        move.start()
    for move in moves:
        move.wait()


def in_hbm(*arrays):
    return [pltpu.with_memory_space_constraint(a, pltpu.HBM) for a in arrays]


def stage(meta, history, taps, *rest, tiles):
    width = tiles * LANES
    arrays = (history, taps) + rest
    shapes = [a.shape[:-1] + (width,) for a in arrays[:2]] + [a.shape for a in rest]
    return pl.pallas_call(
        functools.partial(stage_body, tiles=tiles),
        in_specs=[pl.BlockSpec(memory_space=pltpu.SMEM)]
        + [pl.BlockSpec(memory_space=pltpu.HBM)] * len(arrays),
        out_specs=[pl.BlockSpec(memory_space=pltpu.VMEM)] * len(arrays),
        out_shape=[pltpu.VMEM(d, a.dtype) for d, a in zip(shapes, arrays)],
        scratch_shapes=[
            pltpu.SemaphoreType.DMA((2 * tiles,)),
            pltpu.SemaphoreType.DMA((len(arrays),)),
        ],
        compiler_params=pltpu.CompilerParams(vmem_limit_bytes=16 << 20),
        name="stage",
    )(meta, *in_hbm(*arrays))


def conv_chunk(meta, staged, rim, first, tiles, owners, later=None):
    history, _, _, fwd, _ = staged
    seqs, rows, _ = history.shape
    new = rim.shape[0]
    width = tiles * LANES
    vmem = pl.BlockSpec(memory_space=pltpu.VMEM)
    operands = [meta, *staged, rim]
    in_specs = [pl.BlockSpec(memory_space=pltpu.SMEM)] + [vmem] * 6
    out_shape = [
        jax.ShapeDtypeStruct(
            (seqs, new // 2, width), jnp.bfloat16 if k else jnp.float32
        )
        for k in range(2)
    ]
    scratch = [
        pltpu.VMEM(
            (2, rows // (fwd.shape[1] - new), fwd.shape[0], LANES), jnp.float32
        )
    ]
    base = None
    if later is not None:
        base = tiles
        left = later[0].shape[-1] // LANES - tiles
        operands += in_hbm(*later)
        in_specs += [pl.BlockSpec(memory_space=pltpu.HBM)] * 2
        out_shape += [
            pltpu.VMEM(a.shape[:-1] + (left * LANES,), a.dtype) for a in later
        ]
        scratch.append(pltpu.SemaphoreType.DMA((2 * left,)))
    return pl.pallas_call(
        functools.partial(conv_body, first=first, tiles=tiles, base=base, owners=owners),
        in_specs=in_specs,
        out_specs=[vmem] * len(out_shape),
        out_shape=out_shape,
        scratch_shapes=scratch,
        cost_estimate=pl.CostEstimate(
            flops=2 * width * fwd.shape[0] * rows * (seqs + 1),
            transcendentals=0,
            bytes_accessed=2 * width * rows * (seqs + 1),
        ),
        compiler_params=pltpu.CompilerParams(vmem_limit_bytes=16 << 20),
        name="conv_chunk",
    )(*operands)


def gate_body(gate, *refs, counts):
    *pieces, out = refs
    place = 0
    for count in counts:
        (keep, *got), pieces = pieces[:count], pieces[count:]
        for t in range(keep.shape[2] // LANES):
            here = slice(place * LANES, (place + 1) * LANES)
            there = slice(t * LANES, (t + 1) * LANES)
            value = keep[:, :, there]
            for piece in got:
                value = value + piece[:, :, there].astype(jnp.float32)
            scaled = gate[:, :, here].astype(jnp.float32) * value
            out[:, :, here] = scaled.astype(out.dtype)
            place = place + 1


def gated(gate, chunks):
    vmem = pl.BlockSpec(memory_space=pltpu.VMEM)
    pieces = [piece for chunk in chunks for piece in chunk]
    counts = [len(chunk) for chunk in chunks]
    return pl.pallas_call(
        functools.partial(gate_body, counts=counts),
        in_specs=[vmem] * (1 + len(pieces)),
        out_specs=vmem,
        out_shape=jax.ShapeDtypeStruct(gate.shape, gate.dtype),
        compiler_params=pltpu.CompilerParams(vmem_limit_bytes=16 << 20),
        name="gated",
    )(gate, *pieces)


def chunk_tiles(total):
    parts = min(CHUNKS, total)
    return [total // parts + (index < total % parts) for index in range(parts)]


def swapped(ranks):
    order = [0]
    step = ranks // 2
    while step:
        order += [step ^ value for value in order]
        step //= 2
    return order


def exchange(value, bit, ranks):
    return lax.ppermute(value, "hist", [(z, z ^ bit) for z in range(ranks)])


def body(history, filter_taps, skip_gain, gate_values):
    ranks = lax.axis_size("hist")
    rank = lax.axis_index("hist").astype(jnp.int32)
    share = gate_values.shape[1]
    new = share * ranks
    channels = history.shape[2]
    total = channels // LANES
    block = min(BLOCK, history.shape[1])
    taps_table, back_table = tables(block, new)
    fwd = jnp.asarray(taps_table, jnp.bfloat16)
    order = swapped(ranks)
    by_owner = back_table.reshape(ranks, share, -1)
    turned = np.stack(
        [np.concatenate([by_owner[z ^ j] for j in order]) for z in range(ranks)]
    )
    back = jnp.asarray(turned, jnp.bfloat16)
    owners = [(ranks - 1) ^ j for j in order]
    meta = rank[None]
    sizes = chunk_tiles(total)
    toward = [(source, source - 1) for source in range(1, ranks)]
    split = sizes[0] * LANES
    rims = []
    for part in (slice(0, split), slice(split, None)):
        rims.append(lax.ppermute(filter_taps[:new, part], "hist", toward))
    gain = skip_gain[None, :]
    staged = stage(meta, history, filter_taps, gain, fwd, back, tiles=sizes[0])
    chunks = []
    start = 0
    for index, tiles in enumerate(sizes):
        at = start - sizes[0] if index else 0
        later = None if index or len(sizes) == 1 else (history, filter_taps)
        keep, *sends = conv_chunk(
            meta,
            staged,
            rims[min(index, 1)],
            (at, at, start),
            tiles,
            owners,
            later,
        )
        if later is not None:
            staged = [sends[-2], sends[-1], *staged[2:]]
            sends = sends[:-2]
        bit = 1
        while True:
            got = exchange(sends[0], bit, ranks)
            bit *= 2
            if bit >= ranks:
                break
            summed = keep + got.astype(jnp.float32)
            half = summed.shape[1] // 2
            keep, sends = summed[:, :half], [summed[:, half:].astype(jnp.bfloat16)]
        chunks.append([keep, got])
        start += tiles
    return gated(gate_values, chunks)


def solution(mesh):
    placed = (
        P(("grp", "seq"), "hist", "chan"),
        P(("grp", "hist"), "chan"),
        P(("grp", "chan")),
        P(("grp", "seq"), "hist", "chan"),
    )
    return jax.shard_map(
        body,
        mesh=mesh,
        in_specs=placed,
        out_specs=P(("grp", "seq"), "hist", "chan"),
        check_vma=False,
    )
```

```python
import functools

import jax
import jax.numpy as jnp
import numpy as np
from jax import lax
from jax.experimental import pallas as pl
from jax.experimental.pallas import tpu as pltpu
from jax.sharding import PartitionSpec as P


LANES = 256
BLOCK = 128
CHUNKS = 3
GROUP = 32


def tables(block, new):
    length = block + new
    bins = length // 2
    freq = np.arange(bins)[:, None] + 0.5
    step = 2.0 * np.pi / length

    def pair(positions):
        angle = step * freq * positions[None, :]
        return np.concatenate([np.cos(angle), np.sin(angle)], axis=0)

    taps = pair(np.arange(length))
    back = pair(new - 1 - np.arange(new)).T * (2.0 / length)
    back[:, bins:] *= -1.0
    return taps, back


def moves_in(sources, targets, done, first, count):
    moves = []
    for source, target in zip(sources, targets):
        for t in range(count):
            lead = (slice(None),) * (len(source.shape) - 1)
            there = lead + (pl.ds((first + t) * LANES, LANES),)
            here = lead + (pl.ds(t * LANES, LANES),)
            moves.append(
                pltpu.make_async_copy(source.at[there], target.at[here], done.at[len(moves)])
            )
    return moves


def conv_body(meta, hist, taps, gain, fwd, back, rim, *refs, first, tiles, base, owners):
    if base is None:
        sources, refs = (), refs
        outs, (spectra,) = refs[:-1], refs[-1:]
    else:
        sources, refs = refs[:2], refs[2:]
        outs, targets, (spectra, done) = refs[:-4], refs[-4:-2], refs[-2:]
        later = moves_in(sources, targets, done, base, targets[0].shape[2] // LANES)
        for move in later:
            move.start()
    seqs, rows, _ = hist.shape
    new = rim.shape[0]
    length = fwd.shape[1]
    block = length - new
    bins = length // 2
    count = rows // block
    share = new // len(owners)
    flag = (meta[0] == len(owners) - 1).astype(jnp.float32)
    hist_at, rim_at, gain_at = first

    fwd_taps = fwd[...]
    fwd_hist = fwd[:, :block]
    back_table = back[meta[0]]

    def lanes(tile):
        return slice(tile * LANES, (tile + 1) * LANES)

    def transform(t):
        for q in range(count):
            here = lanes(hist_at + t)
            if q + 1 < count:
                window = taps[q * block : q * block + length, here]
            else:
                window = jnp.concatenate(
                    [taps[q * block :, here], rim[:, lanes(rim_at + t)]], axis=0
                )
            spectra[t % 2, q] = jnp.dot(
                fwd_taps, window, preferred_element_type=jnp.float32
            )

    def forward(t, b):
        return [
            jnp.dot(
                fwd_hist,
                hist[b, q * block : (q + 1) * block, lanes(hist_at + t)],
                preferred_element_type=jnp.float32,
            )
            for q in range(count)
        ]

    def combine(t, data):
        real, imag = [], []
        for f in range(0, bins, GROUP):
            re = im = None
            for q in range(count):
                dc, ds = data[q][f : f + GROUP], data[q][bins + f : bins + f + GROUP]
                tc = spectra[t % 2, q, f : f + GROUP, :]
                ts = spectra[t % 2, q, bins + f : bins + f + GROUP, :]
                now_re, now_im = dc * tc + ds * ts, ds * tc - dc * ts
                re = now_re if re is None else re + now_re
                im = now_im if im is None else im + now_im
            real.append(re.astype(jnp.bfloat16))
            imag.append(im.astype(jnp.bfloat16))
        both = jnp.concatenate(real + imag, axis=0)
        return jnp.dot(back_table, both, preferred_element_type=jnp.float32)

    def finish(t, b, part):
        scale = gain[:, lanes(gain_at + t)] * flag
        newest = hist[b, rows - new :, lanes(hist_at + t)].astype(jnp.float32)
        for k, owner in enumerate(owners):
            direct = scale * newest[owner * share : (owner + 1) * share]
            piece = part[k * share : (k + 1) * share] + direct
            out = outs[k * len(outs) // len(owners)]
            at = k % (len(owners) // len(outs)) * share
            out[b, at : at + share, lanes(t)] = piece.astype(out.dtype)

    def compute():
        steps = [(t, b) for t in range(tiles) for b in range(seqs)]
        transform(0)
        data = forward(*steps[0])
        last = None
        for index, (t, b) in enumerate(steps):
            after = None
            if index + 1 < len(steps):
                if b == seqs // 2 and t + 1 < tiles:
                    transform(t + 1)
                after = forward(*steps[index + 1])
            now = combine(t, data)
            if last is not None:
                finish(*last)
            last, data = (t, b, now), after
        finish(*last)

    if base is None:
        compute()
        return
    pl.when(meta[0] >= 0)(compute)
    for move in later:
        move.wait()


def stage_body(meta, *refs, tiles):
    del meta
    count = len(refs) // 2 - 1
    arrays, copies, (done, whole) = refs[:count], refs[count:-2], refs[-2:]
    moves = moves_in(arrays[:2], copies[:2], done, 0, tiles)
    for i in range(2, count):
        moves.append(pltpu.make_async_copy(arrays[i], copies[i], whole.at[i]))
    for move in moves:
        move.start()
    for move in moves:
        move.wait()


def in_hbm(*arrays):
    return [pltpu.with_memory_space_constraint(a, pltpu.HBM) for a in arrays]


def cut_body(taps, *refs):
    pieces, done = refs[:-1], refs[-1]
    moves = []
    start = 0
    for piece in pieces:
        rows, width = piece.shape
        source = taps.at[pl.ds(0, rows), pl.ds(start, width)]
        moves.append(pltpu.make_async_copy(source, piece, done.at[len(moves)]))
        start += width
    for move in moves:
        move.start()
    for move in moves:
        move.wait()


def cut(taps, rows, widths):
    return pl.pallas_call(
        cut_body,
        in_specs=[pl.BlockSpec(memory_space=pltpu.HBM)],
        out_specs=[pl.BlockSpec(memory_space=pltpu.VMEM)] * len(widths),
        out_shape=[pltpu.VMEM((rows, width), taps.dtype) for width in widths],
        scratch_shapes=[pltpu.SemaphoreType.DMA((len(widths),))],
        compiler_params=pltpu.CompilerParams(vmem_limit_bytes=16 << 20),
        name="cut",
    )(*in_hbm(taps))


def stage(meta, history, taps, *rest, tiles):
    width = tiles * LANES
    arrays = (history, taps) + rest
    shapes = [a.shape[:-1] + (width,) for a in arrays[:2]] + [a.shape for a in rest]
    return pl.pallas_call(
        functools.partial(stage_body, tiles=tiles),
        in_specs=[pl.BlockSpec(memory_space=pltpu.SMEM)]
        + [pl.BlockSpec(memory_space=pltpu.HBM)] * len(arrays),
        out_specs=[pl.BlockSpec(memory_space=pltpu.VMEM)] * len(arrays),
        out_shape=[pltpu.VMEM(d, a.dtype) for d, a in zip(shapes, arrays)],
        scratch_shapes=[
            pltpu.SemaphoreType.DMA((2 * tiles,)),
            pltpu.SemaphoreType.DMA((len(arrays),)),
        ],
        compiler_params=pltpu.CompilerParams(vmem_limit_bytes=16 << 20),
        name="stage",
    )(meta, *in_hbm(*arrays))


def conv_chunk(meta, staged, rim, first, tiles, owners, later=None):
    history, _, _, fwd, _ = staged
    seqs, rows, _ = history.shape
    new = rim.shape[0]
    width = tiles * LANES
    vmem = pl.BlockSpec(memory_space=pltpu.VMEM)
    operands = [meta, *staged, rim]
    in_specs = [pl.BlockSpec(memory_space=pltpu.SMEM)] + [vmem] * 6
    out_shape = [
        jax.ShapeDtypeStruct(
            (seqs, new // 2, width), jnp.bfloat16 if k else jnp.float32
        )
        for k in range(2)
    ]
    scratch = [
        pltpu.VMEM(
            (2, rows // (fwd.shape[1] - new), fwd.shape[0], LANES), jnp.float32
        )
    ]
    base = None
    if later is not None:
        base = tiles
        left = later[0].shape[-1] // LANES - tiles
        operands += in_hbm(*later)
        in_specs += [pl.BlockSpec(memory_space=pltpu.HBM)] * 2
        out_shape += [
            pltpu.VMEM(a.shape[:-1] + (left * LANES,), a.dtype) for a in later
        ]
        scratch.append(pltpu.SemaphoreType.DMA((2 * left,)))
    return pl.pallas_call(
        functools.partial(conv_body, first=first, tiles=tiles, base=base, owners=owners),
        in_specs=in_specs,
        out_specs=[vmem] * len(out_shape),
        out_shape=out_shape,
        scratch_shapes=scratch,
        cost_estimate=pl.CostEstimate(
            flops=2 * width * fwd.shape[0] * rows * (seqs + 1),
            transcendentals=0,
            bytes_accessed=2 * width * rows * (seqs + 1),
        ),
        compiler_params=pltpu.CompilerParams(vmem_limit_bytes=16 << 20),
        name="conv_chunk",
    )(*operands)


def gate_body(gate, *refs, counts):
    *pieces, out = refs
    place = 0
    for count in counts:
        (keep, *got), pieces = pieces[:count], pieces[count:]
        for t in range(keep.shape[2] // LANES):
            here = slice(place * LANES, (place + 1) * LANES)
            there = slice(t * LANES, (t + 1) * LANES)
            value = keep[:, :, there]
            for piece in got:
                value = value + piece[:, :, there].astype(jnp.float32)
            scaled = gate[:, :, here].astype(jnp.float32) * value
            out[:, :, here] = scaled.astype(out.dtype)
            place = place + 1


def gated(gate, chunks):
    vmem = pl.BlockSpec(memory_space=pltpu.VMEM)
    pieces = [piece for chunk in chunks for piece in chunk]
    counts = [len(chunk) for chunk in chunks]
    return pl.pallas_call(
        functools.partial(gate_body, counts=counts),
        in_specs=[vmem] * (1 + len(pieces)),
        out_specs=vmem,
        out_shape=jax.ShapeDtypeStruct(gate.shape, gate.dtype),
        compiler_params=pltpu.CompilerParams(vmem_limit_bytes=16 << 20),
        name="gated",
    )(gate, *pieces)


def chunk_tiles(total):
    parts = min(CHUNKS, total)
    return [total // parts + (index < total % parts) for index in range(parts)]


def swapped(ranks):
    order = [0]
    step = ranks // 2
    while step:
        order += [step ^ value for value in order]
        step //= 2
    return order


def exchange(value, bit, ranks):
    return lax.ppermute(value, "hist", [(z, z ^ bit) for z in range(ranks)])


def body(history, filter_taps, skip_gain, gate_values):
    ranks = lax.axis_size("hist")
    rank = lax.axis_index("hist").astype(jnp.int32)
    share = gate_values.shape[1]
    new = share * ranks
    channels = history.shape[2]
    total = channels // LANES
    block = min(BLOCK, history.shape[1])
    taps_table, back_table = tables(block, new)
    fwd = jnp.asarray(taps_table, jnp.bfloat16)
    order = swapped(ranks)
    by_owner = back_table.reshape(ranks, share, -1)
    turned = np.stack(
        [np.concatenate([by_owner[z ^ j] for j in order]) for z in range(ranks)]
    )
    back = jnp.asarray(turned, jnp.bfloat16)
    owners = [(ranks - 1) ^ j for j in order]
    meta = rank[None]
    sizes = chunk_tiles(total)
    toward = [(source, source - 1) for source in range(1, ranks)]
    split = sizes[0] * LANES
    widths = [split, channels - split] if split < channels else [split]
    rims = []
    for part in cut(filter_taps, new, widths):
        rims.append(lax.ppermute(part, "hist", toward))
    gain = skip_gain[None, :]
    staged = stage(meta, history, filter_taps, gain, fwd, back, tiles=sizes[0])
    chunks = []
    start = 0
    for index, tiles in enumerate(sizes):
        at = start - sizes[0] if index else 0
        later = None if index or len(sizes) == 1 else (history, filter_taps)
        keep, *sends = conv_chunk(
            meta,
            staged,
            rims[min(index, 1)],
            (at, at, start),
            tiles,
            owners,
            later,
        )
        if later is not None:
            staged = [sends[-2], sends[-1], *staged[2:]]
            sends = sends[:-2]
        bit = 1
        while True:
            got = exchange(sends[0], bit, ranks)
            bit *= 2
            if bit >= ranks:
                break
            summed = keep + got.astype(jnp.float32)
            half = summed.shape[1] // 2
            keep, sends = summed[:, :half], [summed[:, half:].astype(jnp.bfloat16)]
        chunks.append([keep, got])
        start += tiles
    return gated(gate_values, chunks)


def solution(mesh):
    placed = (
        P(("grp", "seq"), "hist", "chan"),
        P(("grp", "hist"), "chan"),
        P(("grp", "chan")),
        P(("grp", "seq"), "hist", "chan"),
    )
    return jax.shard_map(
        body,
        mesh=mesh,
        in_specs=placed,
        out_specs=P(("grp", "seq"), "hist", "chan"),
        check_vma=False,
    )
```
